32 devices in a mesh: row: 8 (over y, x, core), col: 4 (over z).
Axes of the slice: x: 2, y: 2, z: 4, core: 2. Of those that a mesh axis runs over, the one named last changes fastest.
Arguments:
- expression: bfloat16 [4096, 1024], P(('row', 'col')), may hold values from -200 to 200, as said below
- powers: int32 [10], replicated, may hold values from 1 to 20
Outputs:
- log_degree: float32 [10, 4096], P(None, ('row', 'col'))
- degree_freq: float32 [10, 10], replicated
- fit_slope: float32 [10], replicated
- mean_log: float32 [10], replicated
The draws below stay inside these ranges and needn't reach their ends.
Inputs may be any that keep to these rules, and one draw needn't show every extreme that they name: Finite expression values.
All inputs are finite; a program needn't handle non-finite values.
Results may differ from the reference program's by a relative error of at most 0.0003.
Values may be sent and summed in bfloat16 or wider, within the bound.
No kernel may reach another device: no remote copies, remote signals or barrier semaphores. Data moves between devices by JAX's collectives and lax.ppermute only.
A program may use at most 64 MiB of HBM per device.

```python
import math
import jax
import jax.numpy as jnp
from jax import lax

S = 1024
NPOW = 10
BINS = 10
MODULES = 400
GENES = 4096


def draw_expression(key, part):
    keys = jax.random.split(key, 10)
    leading_count = max(MODULES // 8, 1)
    leading_ids = jax.random.randint(keys[0], (GENES, 1), 0, leading_count)
    other_ids = jax.random.randint(keys[8], (GENES, 7), 0, MODULES)
    factor_ids = jnp.concatenate([leading_ids, other_ids], axis=1)
    live_count = jax.random.randint(keys[1], (GENES, 1), 1, 6)
    slot_index = jnp.arange(8, dtype=jnp.int32)[None, :]
    leading_strength = jax.random.uniform(keys[2], (GENES, 1), jnp.float32, 0.85, 1.0)
    other_strength = jax.random.uniform(keys[9], (GENES, 7), jnp.float32, 0.1, 0.3)
    strength = jnp.concatenate([leading_strength, other_strength], axis=1)
    signs = (jax.random.randint(keys[3], (GENES, 8), 0, 2) * 2 - 1).astype(jnp.float32)
    loading = jnp.where(slot_index < live_count, strength * signs, 0.0)
    factors = jax.random.normal(keys[4], (MODULES, S), jnp.float32)
    signal = jnp.zeros((GENES, S), jnp.float32)
    for slot in range(8):
        signal = signal + loading[:, slot:slot + 1] * jnp.take(factors, factor_ids[:, slot], axis=0)
    noise_scale = jnp.exp(jax.random.uniform(keys[5], (GENES, 1), jnp.float32, -3.0, 1.0))
    noise_part = jax.random.normal(keys[6], (GENES, S), jnp.float32)
    total = jnp.sum(loading * loading, axis=1, keepdims=True) + noise_scale * noise_scale
    values = (signal + noise_scale * noise_part) / jnp.sqrt(total)
    return values.astype(jnp.bfloat16)


def place_ends(result, own_key, least, top_value):
    shape = result.shape
    spot = [jax.random.randint(jax.random.fold_in(own_key, axis), (), 0, shape[axis]) for axis in range(len(shape))]
    result = result.at[tuple(spot)].set(least)
    longest = shape.index(max(shape))
    spot[longest] = (spot[longest] + 1) % shape[longest]
    return result.at[tuple(spot)].set(top_value)


def setup_inputs(seed: int = 0) -> dict:
    arg_keys = jax.random.split(jax.random.key(seed), 3)
    expression = draw_expression(jax.random.fold_in(arg_keys[2], 71), 0)
    powers = place_ends(jax.random.randint(arg_keys[1], (NPOW,), 1, 21), jax.random.fold_in(arg_keys[1], 1), 1, 20).astype(jnp.int32)
    return dict(expression=expression, powers=powers)


def reference(expression, powers):
    values = expression.astype(jnp.float32)
    gene_mean = lax.optimization_barrier(jnp.mean(values, axis=1))
    centred = values - gene_mean[:, None]
    gene_inv = lax.rsqrt(lax.optimization_barrier(jnp.mean(centred * centred, axis=1)) + 1e-06)
    exponents = powers.astype(jnp.float32)
    block_rows = math.gcd(GENES, 512)
    blocks = GENES // block_rows

    def one_block(packed):
        row_block, block_mean, block_inv = packed
        raw = jnp.dot(row_block, expression.T, preferred_element_type=jnp.float32)
        pearson = (raw / S - block_mean[:, None] * gene_mean[None, :]) * block_inv[:, None] * gene_inv[None, :]
        log_abs = jnp.log(jnp.abs(pearson))
        return jnp.stack([lax.optimization_barrier(jnp.sum(jnp.exp(exponents[power_index] * log_abs), axis=1)) for power_index in range(NPOW)])
    blocked = lax.map(one_block, (expression.reshape(blocks, block_rows, S), gene_mean.reshape(blocks, block_rows), gene_inv.reshape(blocks, block_rows)))
    degree = jnp.transpose(blocked, (1, 0, 2)).reshape(NPOW, GENES)
    peak = lax.optimization_barrier(jnp.max(degree, axis=1))
    position = jnp.clip(BINS * degree / peak[:, None] - 0.5, 0.0, BINS - 1.0)
    centres = jnp.arange(BINS, dtype=jnp.float32)
    weights = jnp.maximum(0.0, 1.0 - jnp.abs(position[:, :, None] - centres[None, None, :]))
    degree_freq = lax.optimization_barrier(jnp.sum(weights, axis=1)) / GENES
    mean_log = jnp.log10(lax.optimization_barrier(jnp.sum(degree, axis=1)) / GENES)
    xfit = jnp.log10((centres[None, :] + 0.5) * peak[:, None] / BINS)
    yfit = jnp.log10(degree_freq + 1.0 / GENES)
    xdev = xfit - lax.optimization_barrier(jnp.mean(xfit, axis=1, keepdims=True))
    ydev = yfit - lax.optimization_barrier(jnp.mean(yfit, axis=1, keepdims=True))
    fit_slope = lax.optimization_barrier(jnp.sum(xdev * ydev, axis=1)) / lax.optimization_barrier(jnp.sum(xdev * xdev, axis=1))
    return (jnp.log10(degree), degree_freq, fit_slope, mean_log)
```

```python
import functools

import jax
import jax.numpy as jnp
from jax import lax
from jax.experimental import pallas as pl
from jax.experimental.pallas import tpu as pltpu
from jax.sharding import PartitionSpec as P

BINS = 10
AXES = ("row", "col")
LOG2E = 1.4426950408889634
LOG10E = 0.4342944819032518


def gene_stats(genes):
    values = genes.astype(jnp.float32)
    samples = values.shape[1]
    mean = jnp.sum(values, axis=1, keepdims=True) * (1.0 / samples)
    centred = values - mean
    var = jnp.sum(centred * centred, axis=1, keepdims=True) * (1.0 / samples)
    return mean, lax.rsqrt(var + 1e-06)


def as_row(column):
    genes = column.shape[0]
    return jnp.transpose(jnp.broadcast_to(column, (genes, genes)))[0:1, :]


def degree_kernel(lane_count, sub_count, prior_count, *refs):
    powers = refs[0]
    lanes = refs[1 : 1 + lane_count]
    subs = refs[1 + lane_count : 1 + lane_count + sub_count]
    prior = refs[1 + lane_count + sub_count] if prior_count else None
    out, raw, lane_mean, lane_inv, acc = refs[-5:]
    npower = powers.shape[0]
    genes, samples = lanes[0].shape
    for a in range(lane_count):
        mean, inv = gene_stats(lanes[a][...])
        lane_mean[a] = jnp.broadcast_to(as_row(mean), (8, genes))
        lane_inv[a] = jnp.broadcast_to(as_row(inv), (8, genes))
    acc[...] = jnp.zeros_like(acc)
    for b in range(sub_count):
        block = subs[b][...]
        mean, inv = gene_stats(block)
        mean = jnp.broadcast_to(mean * samples, (genes, genes))
        inv = jnp.broadcast_to(inv * (1.0 / samples), (genes, genes))
        for a in range(lane_count):
            raw[a] = lax.dot_general(
                block, lanes[a][...], (((1,), (1,)), ((), ())), preferred_element_type=jnp.float32
            )

        def one_tile(a, carry):
            pearson = (raw[a] - mean * lane_mean[a, 0:1, :]) * inv * lane_inv[a, 0:1, :]
            log_abs = jnp.log(jnp.abs(pearson))
            for p in range(npower):
                scale = powers[p].astype(jnp.float32) * LOG2E
                term = jnp.exp2(log_abs * scale)
                acc[a, p] += jnp.sum(term.reshape(genes // 8, 8, genes), axis=0)
            return carry

        lax.fori_loop(0, lane_count, one_tile, 0)
    for s in range(prior_count):
        out[s] = prior[s]
    for a in range(lane_count):
        for p in range(npower):
            out[prior_count + a, p : p + 1, :] = jnp.sum(acc[a, p], axis=0, keepdims=True)


def degrees(powers, lane_blocks, sub_blocks, prior=None):
    npower = powers.shape[0]
    genes, samples = lane_blocks[0].shape
    count = len(lane_blocks)
    prior_count = 0 if prior is None else prior.shape[0]
    pairs = count * len(sub_blocks) * genes * genes
    vmem = pl.BlockSpec(memory_space=pltpu.VMEM)
    operands = list(lane_blocks) + list(sub_blocks) + ([] if prior is None else [prior])
    return pl.pallas_call(
        functools.partial(degree_kernel, count, len(sub_blocks), prior_count),
        out_shape=jax.ShapeDtypeStruct((prior_count + count, npower, genes), jnp.float32),
        in_specs=[pl.BlockSpec(memory_space=pltpu.SMEM)] + [vmem] * len(operands),
        out_specs=vmem,
        scratch_shapes=[
            pltpu.VMEM((count, genes, genes), jnp.float32),
            pltpu.VMEM((count, 8, genes), jnp.float32),
            pltpu.VMEM((count, 8, genes), jnp.float32),
            pltpu.VMEM((count, npower, 8, genes), jnp.float32),
        ],
        cost_estimate=pl.CostEstimate(
            flops=2 * pairs * samples,
            bytes_accessed=2 * genes * samples * len(operands),
            transcendentals=pairs * (npower + 1),
        ),
    )(powers, *operands)


def fit_kernel(place, deg, log_degree, degree_freq, fit_slope, mean_log):
    slots, npower, genes = deg.shape
    inv_genes = 1.0 / (slots * genes)
    start = place[0]
    log_degree[...] = jnp.log(deg[0]) * LOG10E
    top = deg[0]
    for s in range(1, slots):
        top = jnp.maximum(top, deg[s])
    peak = jnp.max(top, axis=1, keepdims=True)
    total = jnp.zeros((npower, genes), jnp.float32)
    counts = [jnp.zeros((npower, genes), jnp.float32) for _ in range(BINS)]
    for s in range(slots):
        value = deg[s ^ start]
        total = total + value
        position = jnp.clip(BINS * value / peak - 0.5, 0.0, BINS - 1.0)
        for b in range(BINS):
            counts[b] = counts[b] + jnp.maximum(0.0, 1.0 - jnp.abs(position - b))
    lane = lax.broadcasted_iota(jnp.int32, (npower, genes), 1)
    freq = jnp.zeros((npower, genes), jnp.float32)
    for b in range(BINS):
        freq = jnp.where(lane == b, jnp.sum(counts[b], axis=1, keepdims=True) * inv_genes, freq)
    degree_freq[...] = freq[:, :BINS]
    mean_col = jnp.log(jnp.sum(total, axis=1, keepdims=True) * inv_genes) * LOG10E
    used = lane < BINS
    centre = lane.astype(jnp.float32) + 0.5
    xfit = jnp.where(used, jnp.log(centre * peak * (1.0 / BINS)) * LOG10E, 0.0)
    yfit = jnp.where(used, jnp.log(freq + inv_genes) * LOG10E, 0.0)
    xdev = jnp.where(used, xfit - jnp.sum(xfit, axis=1, keepdims=True) * (1.0 / BINS), 0.0)
    ydev = jnp.where(used, yfit - jnp.sum(yfit, axis=1, keepdims=True) * (1.0 / BINS), 0.0)
    slope_col = jnp.sum(xdev * ydev, axis=1, keepdims=True) / jnp.sum(
        xdev * xdev, axis=1, keepdims=True
    )
    row = lax.broadcasted_iota(jnp.int32, (npower, genes), 0)
    fit_slope[...] = jnp.sum(jnp.where(lane == row, slope_col, 0.0), axis=0, keepdims=True)[
        :, :npower
    ]
    mean_log[...] = jnp.sum(jnp.where(lane == row, mean_col, 0.0), axis=0, keepdims=True)[
        :, :npower
    ]


def fit(place, deg):
    slots, npower, genes = deg.shape
    vmem = pl.BlockSpec(memory_space=pltpu.VMEM)
    return pl.pallas_call(
        fit_kernel,
        out_shape=(
            jax.ShapeDtypeStruct((npower, genes), jnp.float32),
            jax.ShapeDtypeStruct((npower, BINS), jnp.float32),
            jax.ShapeDtypeStruct((1, npower), jnp.float32),
            jax.ShapeDtypeStruct((1, npower), jnp.float32),
        ),
        in_specs=[pl.BlockSpec(memory_space=pltpu.SMEM), vmem],
        out_specs=(vmem,) * 4,
    )(place, deg)


def bits_of(low, high):
    bits = []
    while low < high:
        bits.append(low)
        low *= 2
    return bits


def on_device(expression, powers):
    rows, cols = lax.axis_size("row"), lax.axis_size("col")
    devices = rows * cols
    me = lax.axis_index(AXES)

    def from_partner(array, bit):
        return lax.ppermute(array, AXES, [(i, i ^ bit) for i in range(devices)])

    col_bits, row_bits = bits_of(1, cols), bits_of(2 * cols, devices)
    core_bit = cols
    far = col_bits[len(col_bits) // 2 :] + row_bits[len(row_bits) // 2 :]
    near = col_bits[: len(col_bits) // 2] + row_bits[: len(row_bits) // 2]

    lane_blocks = [(0, expression)]
    for bit in far:
        lane_blocks += [(mask ^ bit, from_partner(block, bit)) for mask, block in lane_blocks]
    sub_blocks = [expression]
    for bit in near:
        sub_blocks += [from_partner(block, bit) for block in sub_blocks]
    sub_blocks += [from_partner(block, core_bit) for block in sub_blocks]

    split = len(lane_blocks) - max(len(lane_blocks) // 4, 1)
    masks = [mask for mask, _ in lane_blocks]
    blocks = [block for _, block in lane_blocks]
    part = degrees(powers, blocks[:split], sub_blocks)
    part = degrees(powers, blocks[split:], sub_blocks, part)

    for bit in far:
        order = [masks.index(mask ^ bit) for mask in masks]
        received = from_partner(part, bit)
        part = part + jnp.stack([received[s] for s in order])
    for bit in near + [core_bit]:
        part = jnp.concatenate([part, from_partner(part, bit)])
        masks = masks + [mask ^ bit for mask in masks]

    place = jnp.zeros((), jnp.int32)
    slot = 1
    while slot < devices:
        place = place | jnp.where(me & masks[slot] != 0, slot, 0)
        slot *= 2
    log_degree, degree_freq, fit_slope, mean_log = fit(place[None], part)
    return log_degree, degree_freq, fit_slope[0], mean_log[0]


def solution(mesh):
    return jax.shard_map(
        on_device,
        mesh=mesh,
        in_specs=(P(AXES, None), P()),
        out_specs=(P(None, AXES), P(), P(), P()),
        check_vma=False,
    )
```

```python
import functools

import jax
import jax.numpy as jnp
from jax import lax
from jax.experimental import pallas as pl
from jax.experimental.pallas import tpu as pltpu
from jax.sharding import PartitionSpec as P


BINS = 10
AXES = ("row", "col")
LOG2E = 1.4426950408889634
LOG10E = 0.4342944819032518
TILE = 8
VMEM_LIMIT = 20 * 2**20


def gene_stats(genes):
    values = genes.astype(jnp.float32)
    samples = values.shape[1]
    mean = jnp.sum(values, axis=1, keepdims=True) * (1.0 / samples)
    centred = values - mean
    var = jnp.sum(centred * centred, axis=1, keepdims=True) * (1.0 / samples)
    return mean, lax.rsqrt(var + 1e-06)


def as_row(column):
    genes = column.shape[0]
    return jnp.transpose(jnp.broadcast_to(column, (genes, genes)))[0:1, :]


def vmem_spec():
    return pl.BlockSpec(memory_space=pltpu.VMEM)


def smem_spec():
    return pl.BlockSpec(memory_space=pltpu.SMEM)


def stats_kernel(count, *refs):
    out = refs[-1]
    for b in range(count):
        genes, samples = refs[b].shape
        mean, inv = gene_stats(refs[b][...])
        out[b, 0] = jnp.broadcast_to(mean * samples, (genes, genes))
        out[b, 1] = jnp.broadcast_to(inv * (1.0 / samples), (genes, genes))


def stats(blocks):
    genes = blocks[0].shape[0]
    return pl.pallas_call(
        functools.partial(stats_kernel, len(blocks)),
        out_shape=jax.ShapeDtypeStruct((len(blocks), 2, genes, genes), jnp.float32),
        in_specs=[vmem_spec()] * len(blocks),
        out_specs=vmem_spec(),
        compiler_params=pltpu.CompilerParams(vmem_limit_bytes=VMEM_LIMIT),
        cost_estimate=pl.CostEstimate(
            flops=400000 * len(blocks), bytes_accessed=400000 * len(blocks), transcendentals=0
        ),
    )(*blocks)


def add_powers(powers, lane_refs, sub_refs, stat_refs, raw, emit):
    npower = powers.shape[0]
    genes, _ = lane_refs[0].shape
    chunk = 32
    scales = [powers[p].astype(jnp.float32) * LOG2E for p in range(npower)]

    def one_lane_block(a, lane_ref):
        mean, inv = gene_stats(lane_ref[...])
        lane_mean, lane_inv = as_row(mean), as_row(inv)
        for b, sub_ref in enumerate(sub_refs):
            raw[b] = lax.dot_general(
                sub_ref[...],
                lane_ref[...],
                (((1,), (1,)), ((), ())),
                preferred_element_type=jnp.float32,
            )
        sums = [jnp.zeros((TILE, genes), jnp.float32) for _ in range(npower)]
        for b in range(len(sub_refs)):
            for c in range(0, genes, chunk):
                part = slice(c, c + chunk)
                pearson = (
                    (raw[b, part, :] - stat_refs[b][0, part, :] * lane_mean)
                    * stat_refs[b][1, part, :]
                    * lane_inv
                )
                log_abs = jnp.log(jnp.abs(pearson))
                for p in range(npower):
                    term = jnp.exp2(log_abs * scales[p])
                    sums[p] = sums[p] + jnp.sum(
                        term.reshape(chunk // TILE, TILE, genes), axis=0
                    )
        emit(a, [jnp.sum(total, axis=0, keepdims=True) for total in sums])

    for a, lane_ref in enumerate(lane_refs):
        one_lane_block(a, lane_ref)


def early_kernel(lane_count, sub_count, stat_sizes, *refs):
    powers, refs = refs[0], refs[1:]
    lanes, refs = refs[:lane_count], refs[lane_count:]
    subs, refs = refs[:sub_count], refs[sub_count:]
    stat_refs = [refs[i].at[j] for i, size in enumerate(stat_sizes) for j in range(size)]
    out, raw = refs[-2:]

    def emit(a, rows):
        for p, row in enumerate(rows):
            out[a, p : p + 1, :] = row

    add_powers(powers, lanes, subs, stat_refs, raw, emit)


def late_kernel(lane_count, sub_count, stat_sizes, *refs):
    powers, place, refs = refs[0], refs[1], refs[2:]
    lanes, refs = refs[:lane_count], refs[lane_count:]
    subs, refs = refs[:sub_count], refs[sub_count:]
    stat_refs = [refs[i].at[j] for i, size in enumerate(stat_sizes) for j in range(size)]
    prior, out, raw = refs[-3:]
    npower = powers.shape[0]
    genes = lanes[0].shape[0]
    prior_count = prior.shape[0]
    slots = prior_count + lane_count
    full, rest = npower // TILE, npower % TILE
    mine = place[0]
    tail_tiles = out.shape[0] - slots * full
    sublane = lax.broadcasted_iota(jnp.int32, (TILE, genes), 0)
    tail = [jnp.zeros((TILE, genes), jnp.float32) for _ in range(tail_tiles)]

    def emit(slot, rows):
        where = slot ^ mine
        for f in range(full):
            for r in range(TILE):
                out[f * slots + where, r : r + 1, :] = rows[f * TILE + r]
        for q in range(rest):
            for t in range(tail_tiles):
                hit = sublane + t * TILE == q * slots + where
                tail[t] = jnp.where(hit, rows[full * TILE + q], tail[t])

    add_powers(powers, lanes, subs, stat_refs, raw, lambda a, rows: emit(prior_count + a, rows))
    for s in range(prior_count):
        emit(s, [prior[s, p : p + 1, :] for p in range(npower)])
    for t in range(tail_tiles):
        out[slots * full + t] = tail[t]


def tile_count(npower, slots):
    return slots * (npower // TILE) + -(-(npower % TILE) * slots // TILE)


def degrees(powers, lane_blocks, sub_blocks, sub_stats, place=None, prior=None):
    npower = powers.shape[0]
    genes, samples = lane_blocks[0].shape
    lane_count, sub_count = len(lane_blocks), len(sub_blocks)
    pairs = lane_count * sub_count * genes * genes
    operands = list(lane_blocks) + list(sub_blocks) + list(sub_stats)
    scalars = [powers]
    sizes = [array.shape[0] for array in sub_stats]
    if prior is None:
        kernel = early_kernel
        out_shape = (lane_count, npower, genes)
    else:
        kernel = late_kernel
        operands, scalars = operands + [prior], [powers, place]
        out_shape = (tile_count(npower, prior.shape[0] + lane_count), TILE, genes)
    return pl.pallas_call(
        functools.partial(kernel, lane_count, sub_count, sizes),
        out_shape=jax.ShapeDtypeStruct(out_shape, jnp.float32),
        in_specs=[smem_spec()] * len(scalars) + [vmem_spec()] * len(operands),
        out_specs=vmem_spec(),
        scratch_shapes=[pltpu.VMEM((sub_count, genes, genes), jnp.float32)],
        compiler_params=pltpu.CompilerParams(vmem_limit_bytes=VMEM_LIMIT),
        cost_estimate=pl.CostEstimate(
            flops=2 * pairs * samples,
            bytes_accessed=2 * genes * samples * (lane_count + sub_count),
            transcendentals=pairs * (npower + 1),
        ),
    )(*scalars, *operands)


def fit_kernel(npower, slots, place, deg, log_degree, degree_freq, fit_slope, mean_log):
    groups, tiles, _, genes = deg.shape
    full, rest = npower // TILE, npower % TILE
    total_genes = groups * slots * genes
    inv_genes = 1.0 / total_genes
    mine, start = place[0], place[1]
    tail = tiles - slots * full
    sublane = lax.broadcasted_iota(jnp.int32, (TILE, genes), 0)
    lane = lax.broadcasted_iota(jnp.int32, (TILE, genes), 1)
    slope_row, mean_row = 0.0, 0.0

    def hat(value, inverse, counts):
        position = jnp.clip(BINS * value * inverse - 0.5, 0.0, BINS - 1.0)
        return [
            count + jnp.maximum(0.0, 1.0 - jnp.abs(position - b)) for b, count in enumerate(counts)
        ]

    def line(peak, freq, total):
        used = lane < BINS
        centre = lane.astype(jnp.float32) + 0.5
        xfit = jnp.where(used, jnp.log(centre * peak * (1.0 / BINS)) * LOG10E, 0.0)
        yfit = jnp.where(used, jnp.log(freq + inv_genes) * LOG10E, 0.0)
        xdev = jnp.where(used, xfit - jnp.sum(xfit, axis=1, keepdims=True) * (1.0 / BINS), 0.0)
        ydev = jnp.where(used, yfit - jnp.sum(yfit, axis=1, keepdims=True) * (1.0 / BINS), 0.0)
        slope = jnp.sum(xdev * ydev, axis=1, keepdims=True) / jnp.sum(
            xdev * xdev, axis=1, keepdims=True
        )
        return slope, jnp.log(total * inv_genes) * LOG10E

    def on_lanes(counts):
        freq = jnp.zeros((TILE, genes), jnp.float32)
        for b in range(BINS):
            freq = jnp.where(lane == b, counts[b] * inv_genes, freq)
        return freq

    zero = jnp.zeros((TILE, genes), jnp.float32)
    for f in range(full):
        top = deg[0, f * slots]
        for g in range(groups):
            for s in range(slots):
                top = jnp.maximum(top, deg[g, f * slots + s])
        peak = jnp.max(top, axis=1, keepdims=True)
        inverse = 1.0 / peak
        total, counts = zero, [zero] * BINS
        for g in range(groups):
            for s in range(slots):
                value = deg[g ^ start, f * slots + s]
                total = total + value
                counts = hat(value, inverse, counts)
        freq = on_lanes([jnp.sum(count, axis=1, keepdims=True) for count in counts])
        slope, mean = line(peak, freq, jnp.sum(total, axis=1, keepdims=True))
        log_degree[f * TILE : (f + 1) * TILE, :] = jnp.log(deg[0, f * slots + mine]) * LOG10E
        degree_freq[f * TILE : (f + 1) * TILE, :] = freq[:, :BINS]
        diagonal = lane == sublane + f * TILE
        slope_row += jnp.sum(jnp.where(diagonal, slope, 0.0), axis=0, keepdims=True)
        mean_row += jnp.sum(jnp.where(diagonal, mean, 0.0), axis=0, keepdims=True)

    if rest:
        base = slots * full
        row_power = [(sublane + t * TILE) // slots for t in range(tail)]
        row_slot = [(sublane + t * TILE) % slots for t in range(tail)]

        def per_power(columns, combine, neutral):
            whole = [zero for _ in range(tail)]
            for q in range(rest):
                picked = [
                    jnp.where(row_power[t] == q, columns[t], neutral) for t in range(tail)
                ]
                merged = functools.reduce(combine, picked)
                reduce = jnp.max if combine is jnp.maximum else jnp.sum
                value = reduce(merged, axis=0, keepdims=True)
                whole = [jnp.where(row_power[t] == q, value, whole[t]) for t in range(tail)]
            return whole

        tops, totals, counts = [], [], []
        for t in range(tail):
            top = deg[0, base + t]
            for g in range(groups):
                top = jnp.maximum(top, deg[g, base + t])
            tops.append(jnp.max(top, axis=1, keepdims=True))
        peaks = per_power(tops, jnp.maximum, 0.0)
        for t in range(tail):
            inverse = 1.0 / peaks[t]
            total, count = zero, [zero] * BINS
            for g in range(groups):
                value = deg[g ^ start, base + t]
                total = total + value
                count = hat(value, inverse, count)
            totals.append(jnp.sum(total, axis=1, keepdims=True))
            counts.append([jnp.sum(c, axis=1, keepdims=True) for c in count])
        totals = per_power(totals, jnp.add, 0.0)
        freqs = per_power([on_lanes(c) for c in counts], jnp.add, 0.0)
        for q in range(rest):
            t, r = q * slots // TILE, q * slots % TILE
            p = full * TILE + q
            slope, mean = line(peaks[t], freqs[t], totals[t])
            degree_freq[p : p + 1, :] = freqs[t][r : r + 1, :BINS]
            here = (lane == p) & (sublane == r)
            slope_row += jnp.sum(jnp.where(here, slope, 0.0), axis=0, keepdims=True)
            mean_row += jnp.sum(jnp.where(here, mean, 0.0), axis=0, keepdims=True)
            own = zero
            for t in range(tail):
                hit = (row_power[t] == q) & (row_slot[t] == mine)
                own = own + jnp.where(hit, deg[0, base + t], 0.0)
            log_degree[p : p + 1, :] = jnp.log(jnp.sum(own, axis=0, keepdims=True)) * LOG10E
    fit_slope[...] = slope_row[:, :npower]
    mean_log[...] = mean_row[:, :npower]


def fit(npower, slots, place, deg):
    genes = deg.shape[-1]
    return pl.pallas_call(
        functools.partial(fit_kernel, npower, slots),
        out_shape=(
            jax.ShapeDtypeStruct((npower, genes), jnp.float32),
            jax.ShapeDtypeStruct((npower, BINS), jnp.float32),
            jax.ShapeDtypeStruct((1, npower), jnp.float32),
            jax.ShapeDtypeStruct((1, npower), jnp.float32),
        ),
        in_specs=[smem_spec(), vmem_spec()],
        out_specs=(vmem_spec(),) * 4,
        compiler_params=pltpu.CompilerParams(vmem_limit_bytes=VMEM_LIMIT),
    )(place, deg)


def bits_of(low, high):
    bits = []
    while low < high:
        bits.append(low)
        low *= 2
    return bits


def split_bits(rows, cols):
    devices = rows * cols
    col_bits, row_bits = bits_of(1, cols), bits_of(2 * cols, devices)
    far = col_bits[len(col_bits) // 2 :] + row_bits[len(row_bits) // 2 :]
    near = col_bits[: len(col_bits) // 2] + row_bits[: len(row_bits) // 2]
    return [bit ^ cols for bit in far], [bit ^ cols for bit in near]


def on_device(expression, powers):
    rows, cols = lax.axis_size("row"), lax.axis_size("col")
    devices = rows * cols
    npower = powers.shape[0]
    me = lax.axis_index(AXES)
    far, near = split_bits(rows, cols)
    core = cols

    def from_partner(array, bit):
        return lax.ppermute(array, AXES, [(i, i ^ bit) for i in range(devices)])

    def digit(bits, source):
        value = jnp.zeros((), jnp.int32)
        for i, bit in enumerate(bits):
            value = value | jnp.where(source & bit != 0, 1 << i, 0)
        return value

    parity = (me & core) // core
    for bit in far:
        parity = parity ^ jnp.where(me & (bit ^ core) != 0, 1, 0)
    for bit in near:
        parity = parity ^ jnp.where(me & (bit ^ core) != 0, 1, 0)
    mine = digit([bit ^ core for bit in far], me)
    start = digit([bit ^ core for bit in near], me) | parity << len(near)
    place = jnp.stack([mine, start]).astype(jnp.int32)

    lane_blocks = [expression]
    for bit in far:
        lane_blocks += [from_partner(block, bit) for block in lane_blocks]
    sub_blocks = [expression]
    for bit in near:
        sub_blocks += [from_partner(block, bit) for block in sub_blocks]
    sub_blocks += [from_partner(block, core) for block in sub_blocks]

    split = len(lane_blocks) - max(len(lane_blocks) // 4, 1)
    sub_stats = [stats(sub_blocks)]
    part = degrees(powers, lane_blocks[:split], sub_blocks, sub_stats)
    part = degrees(powers, lane_blocks[split:], sub_blocks, sub_stats, place, part)

    for bit in far:
        part = part + from_partner(part, bit)
    part = part[None]
    for bit in near + [core]:
        part = jnp.concatenate([part, from_partner(part, bit)])

    log_degree, degree_freq, fit_slope, mean_log = fit(
        npower, len(lane_blocks), place, part
    )
    return log_degree, degree_freq, fit_slope[0], mean_log[0]


def solution(mesh):
    return jax.shard_map(
        on_device,
        mesh=mesh,
        in_specs=(P(AXES, None), P()),
        out_specs=(P(None, AXES), P(), P(), P()),
        check_vma=False,
    )
```

```python
import functools

import jax
import jax.numpy as jnp
from jax import lax
from jax.experimental import pallas as pl
from jax.experimental.pallas import tpu as pltpu
from jax.sharding import PartitionSpec as P


BINS = 10
AXES = ("row", "col")
LOG2E = 1.4426950408889634
LOG10E = 0.4342944819032518
TILE = 8
CHUNK = 32
PIECES = 2
VMEM_LIMIT = 20 * 2**20


def gene_stats(genes):
    values = genes.astype(jnp.float32)
    samples = values.shape[1]
    mean = jnp.sum(values, axis=1, keepdims=True) * (1.0 / samples)
    centred = values - mean
    var = jnp.sum(centred * centred, axis=1, keepdims=True) * (1.0 / samples)
    return mean, lax.rsqrt(var + 1e-06)


def as_row(column):
    genes = column.shape[0]
    return jnp.transpose(jnp.broadcast_to(column, (genes, genes)))[0:1, :]


def vmem_spec():
    return pl.BlockSpec(memory_space=pltpu.VMEM)


def pallas(kernel, out_shape, operands, scratch=(), cost=None):
    return pl.pallas_call(
        kernel,
        out_shape=out_shape,
        in_specs=[vmem_spec()] * len(operands),
        out_specs=jax.tree.map(lambda _: vmem_spec(), out_shape),
        scratch_shapes=list(scratch),
        compiler_params=pltpu.CompilerParams(vmem_limit_bytes=VMEM_LIMIT),
        cost_estimate=cost,
    )(*operands)


def f32(*shape):
    return jax.ShapeDtypeStruct(shape, jnp.float32)


def split_refs(refs, sizes):
    groups = []
    for size in sizes:
        groups.append(refs[:size])
        refs = refs[size:]
    return groups, refs


def whole(parts):
    return jnp.concatenate([part[...] for part in parts], axis=1)


def measure_sub(block, out):
    genes, samples = block.shape
    mean, inv = gene_stats(block)
    out[0] = jnp.broadcast_to(mean * samples, (genes, genes))
    out[1] = jnp.broadcast_to(inv * (1.0 / samples), (genes, genes))


def row_sums(raw, column, sub_stats, lane_mean, lane_inv, scales):
    npower, _, genes = scales.shape
    sums = [jnp.zeros((TILE, genes), jnp.float32) for _ in range(npower)]
    for b, stat in enumerate(sub_stats):
        for c in range(0, genes, CHUNK):
            part = slice(c, c + CHUNK)
            pearson = (
                (raw[b, part, column] - stat[0, part, :] * lane_mean)
                * stat[1, part, :]
                * lane_inv
            )
            log_abs = jnp.log(jnp.abs(pearson)).reshape(CHUNK // TILE, TILE, genes)
            for p in range(npower):
                term = jnp.exp2(log_abs * scales[p])
                sums[p] = sums[p] + jnp.sum(term, axis=0)
    return [jnp.sum(total, axis=0, keepdims=True) for total in sums]


def multiply(raw, sub_refs, lanes):
    for b, sub_ref in enumerate(sub_refs):
        raw[b] = lax.dot_general(
            sub_ref[...], lanes, (((1,), (1,)), ((), ())), preferred_element_type=jnp.float32
        )


def early_kernel(lane_sizes, sub_count, scales, place, *refs):
    lanes, refs = split_refs(refs, lane_sizes)
    subs, (out, sub_stats, raw) = refs[:sub_count], refs[sub_count:]
    _, _, genes = scales.shape
    blocks = [whole(parts) for parts in lanes]
    multiply(raw, subs, jnp.concatenate(blocks, axis=0))
    for b, sub in enumerate(subs):
        measure_sub(sub[...], sub_stats.at[b])
    stat_refs = [sub_stats.at[b] for b in range(sub_count)]
    for a, block in enumerate(blocks):
        mean, inv = gene_stats(block)
        mean, inv = as_row(mean), as_row(inv)
        column = slice(a * genes, (a + 1) * genes)
        rows = row_sums(raw, column, stat_refs, mean, inv, scales)
        for p, row in enumerate(rows + [mean, inv]):
            out[a, p : p + 1, :] = row


def late_kernel(here_sizes, last_sizes, first_count, second_count, scales, place, *refs):
    here, refs = split_refs(refs, here_sizes)
    last, refs = split_refs(refs, last_sizes)
    (first, second), refs = split_refs(refs, (first_count, second_count))
    first_stats, prior, out, raw_here, raw_last, second_stats = refs
    npower, _, genes = scales.shape
    slots = len(here) + len(last)
    full, rest = npower // TILE, npower % TILE
    second_refs = [second_stats.at[b] for b in range(second_count)]
    all_refs = [first_stats.at[b] for b in range(first_count)] + second_refs
    rows = []
    multiply(raw_here, second, jnp.concatenate([whole(parts) for parts in here], axis=0))
    for b, sub in enumerate(second):
        measure_sub(sub[...], second_stats.at[b])
    blocks = [whole(parts) for parts in last]
    multiply(raw_last, first + second, jnp.concatenate(blocks, axis=0))
    for a in range(len(here)):
        mean, inv = prior[a, npower : npower + 1, :], prior[a, npower + 1 : npower + 2, :]
        column = slice(a * genes, (a + 1) * genes)
        added = row_sums(raw_here, column, second_refs, mean, inv, scales)
        rows.append([row + prior[a, p : p + 1, :] for p, row in enumerate(added)])
    for a, block in enumerate(blocks):
        mean, inv = gene_stats(block)
        column = slice(a * genes, (a + 1) * genes)
        rows.append(row_sums(raw_last, column, all_refs, as_row(mean), as_row(inv), scales))

    mine = place[...]
    sublane = lax.broadcasted_iota(jnp.int32, (TILE, genes), 0)
    for f in range(full):
        for target in range(slots):
            tile = jnp.concatenate(rows[0][f * TILE : (f + 1) * TILE], axis=0)
            for s in range(1, slots):
                other = jnp.concatenate(rows[s][f * TILE : (f + 1) * TILE], axis=0)
                tile = jnp.where(mine == (s ^ target), other, tile)
            out[f * slots + target] = tile
    for t in range(out.shape[0] - full * slots):
        tile = jnp.zeros((TILE, genes), jnp.float32)
        for q in range(rest):
            for s in range(slots):
                hit = sublane + t * TILE == q * slots + (mine ^ s)
                tile = jnp.where(hit, rows[s][full * TILE + q], tile)
        out[full * slots + t] = tile


def tile_count(npower, slots):
    return slots * (npower // TILE) + -(-(npower % TILE) * slots // TILE)


def work(pairs, samples, npower):
    return pl.CostEstimate(
        flops=2 * pairs * samples, bytes_accessed=4 * pairs, transcendentals=pairs * (npower + 1)
    )


def flat(blocks):
    return [part for parts in blocks for part in parts]


def sizes_of(blocks):
    return [len(parts) for parts in blocks]


def early_sums(scales, place, here, first):
    genes, samples = first[0].shape
    npower = scales.shape[0]
    return pallas(
        functools.partial(early_kernel, sizes_of(here), len(first)),
        (f32(len(here), npower + 2, genes), f32(len(first), 2, genes, genes)),
        [scales, place] + flat(here) + first,
        [pltpu.VMEM((len(first), genes, len(here) * genes), jnp.float32)],
        work(len(here) * len(first) * genes * genes, samples, npower),
    )


def late_sums(scales, place, here, last, first, second, first_stats, prior):
    genes, samples = first[0].shape
    npower = scales.shape[0]
    blocks = len(here) * len(second) + len(last) * (len(first) + len(second))
    return pallas(
        functools.partial(
            late_kernel, sizes_of(here), sizes_of(last), len(first), len(second)
        ),
        f32(tile_count(npower, len(here) + len(last)), TILE, genes),
        [scales, place] + flat(here) + flat(last) + first + second + [first_stats, prior],
        [
            pltpu.VMEM((len(second), genes, len(here) * genes), jnp.float32),
            pltpu.VMEM((len(first) + len(second), genes, len(last) * genes), jnp.float32),
            pltpu.VMEM((len(second), 2, genes, genes), jnp.float32),
        ],
        work(blocks * genes * genes, samples, npower),
    )


def fit_kernel(npower, slots, place, deg, own, log_degree, degree_freq, fit_slope, mean_log):
    groups, tiles, _, genes = deg.shape
    full, rest = npower // TILE, npower % TILE
    total_genes = groups * slots * genes
    inv_genes = 1.0 / total_genes
    mine = place[...]
    tail = tiles - slots * full
    sublane = lax.broadcasted_iota(jnp.int32, (TILE, genes), 0)
    lane = lax.broadcasted_iota(jnp.int32, (TILE, genes), 1)
    slope_row, mean_row = 0.0, 0.0

    def hat(value, inverse, counts):
        position = jnp.clip(BINS * value * inverse - 0.5, 0.0, BINS - 1.0)
        return [
            count + jnp.maximum(0.0, 1.0 - jnp.abs(position - b)) for b, count in enumerate(counts)
        ]

    def line(peak, freq, total):
        used = lane < BINS
        centre = lane.astype(jnp.float32) + 0.5
        xfit = jnp.where(used, jnp.log(centre * peak * (1.0 / BINS)) * LOG10E, 0.0)
        yfit = jnp.where(used, jnp.log(freq + inv_genes) * LOG10E, 0.0)
        xdev = jnp.where(used, xfit - jnp.sum(xfit, axis=1, keepdims=True) * (1.0 / BINS), 0.0)
        ydev = jnp.where(used, yfit - jnp.sum(yfit, axis=1, keepdims=True) * (1.0 / BINS), 0.0)
        slope = jnp.sum(xdev * ydev, axis=1, keepdims=True) / jnp.sum(
            xdev * xdev, axis=1, keepdims=True
        )
        return slope, jnp.log(total * inv_genes) * LOG10E

    def on_lanes(counts):
        freq = jnp.zeros((TILE, genes), jnp.float32)
        for b in range(BINS):
            freq = jnp.where(lane == b, counts[b] * inv_genes, freq)
        return freq

    zero = jnp.zeros((TILE, genes), jnp.float32)
    for f in range(full):
        top = deg[0, f * slots]
        for g in range(groups):
            for s in range(slots):
                top = jnp.maximum(top, deg[g, f * slots + s])
        peak = jnp.max(top, axis=1, keepdims=True)
        inverse = 1.0 / peak
        total, counts = zero, [zero] * BINS
        for g in range(groups):
            for s in range(slots):
                value = deg[g, f * slots + s]
                total = total + value
                counts = hat(value, inverse, counts)
        freq = on_lanes([jnp.sum(count, axis=1, keepdims=True) for count in counts])
        slope, mean = line(peak, freq, jnp.sum(total, axis=1, keepdims=True))
        value = own[f * slots]
        for s in range(1, slots):
            value = jnp.where(mine == s, own[f * slots + s], value)
        log_degree[f * TILE : (f + 1) * TILE, :] = jnp.log(value) * LOG10E
        degree_freq[f * TILE : (f + 1) * TILE, :] = freq[:, :BINS]
        diagonal = lane == sublane + f * TILE
        slope_row += jnp.sum(jnp.where(diagonal, slope, 0.0), axis=0, keepdims=True)
        mean_row += jnp.sum(jnp.where(diagonal, mean, 0.0), axis=0, keepdims=True)

    if rest:
        base = slots * full
        row_power = [(sublane + t * TILE) // slots for t in range(tail)]
        row_slot = [(sublane + t * TILE) % slots for t in range(tail)]

        def per_power(columns, combine, neutral):
            whole = [zero for _ in range(tail)]
            for q in range(rest):
                picked = [
                    jnp.where(row_power[t] == q, columns[t], neutral) for t in range(tail)
                ]
                merged = functools.reduce(combine, picked)
                reduce = jnp.max if combine is jnp.maximum else jnp.sum
                value = reduce(merged, axis=0, keepdims=True)
                whole = [jnp.where(row_power[t] == q, value, whole[t]) for t in range(tail)]
            return whole

        tops, totals, counts = [], [], []
        for t in range(tail):
            top = deg[0, base + t]
            for g in range(groups):
                top = jnp.maximum(top, deg[g, base + t])
            tops.append(jnp.max(top, axis=1, keepdims=True))
        peaks = per_power(tops, jnp.maximum, 0.0)
        for t in range(tail):
            inverse = 1.0 / peaks[t]
            total, count = zero, [zero] * BINS
            for g in range(groups):
                value = deg[g, base + t]
                total = total + value
                count = hat(value, inverse, count)
            totals.append(jnp.sum(total, axis=1, keepdims=True))
            counts.append([jnp.sum(c, axis=1, keepdims=True) for c in count])
        totals = per_power(totals, jnp.add, 0.0)
        freqs = per_power([on_lanes(c) for c in counts], jnp.add, 0.0)
        for q in range(rest):
            t, r = q * slots // TILE, q * slots % TILE
            p = full * TILE + q
            slope, mean = line(peaks[t], freqs[t], totals[t])
            degree_freq[p : p + 1, :] = freqs[t][r : r + 1, :BINS]
            here = (lane == p) & (sublane == r)
            slope_row += jnp.sum(jnp.where(here, slope, 0.0), axis=0, keepdims=True)
            mean_row += jnp.sum(jnp.where(here, mean, 0.0), axis=0, keepdims=True)
            value = zero
            for t in range(tail):
                hit = (row_power[t] == q) & (row_slot[t] == mine)
                value = value + jnp.where(hit, own[base + t], 0.0)
            log_degree[p : p + 1, :] = jnp.log(jnp.sum(value, axis=0, keepdims=True)) * LOG10E
    fit_slope[...] = slope_row[:, :npower]
    mean_log[...] = mean_row[:, :npower]


def fit(npower, slots, place, deg, own):
    genes = deg.shape[-1]
    return pallas(
        functools.partial(fit_kernel, npower, slots),
        (f32(npower, genes), f32(npower, BINS), f32(1, npower), f32(1, npower)),
        [place, deg, own],
    )


def bits_of(low, high):
    bits = []
    while low < high:
        bits.append(low)
        low *= 2
    return bits


def split_bits(rows, cols):
    devices = rows * cols
    col_bits, row_bits = bits_of(1, cols), bits_of(2 * cols, devices)
    far = col_bits[len(col_bits) // 2 :] + row_bits[len(row_bits) // 2 :]
    near = col_bits[: len(col_bits) // 2] + row_bits[: len(row_bits) // 2]
    return [bit ^ cols for bit in far], [bit ^ cols for bit in near]


def on_device(expression, powers):
    rows, cols = lax.axis_size("row"), lax.axis_size("col")
    devices = rows * cols
    npower = powers.shape[0]
    me = lax.axis_index(AXES)
    far, near = split_bits(rows, cols)
    core = cols

    def from_partner(array, bit):
        return lax.ppermute(array, AXES, [(i, i ^ bit) for i in range(devices)])

    mine = jnp.zeros((), jnp.int32)
    parity = me & core != 0
    for i, bit in enumerate(far):
        mine = mine | jnp.where(me & (bit ^ core) != 0, 1 << i, 0)
        parity = parity ^ (me & (bit ^ core) != 0)
    upper = []
    for bit in near:
        upper.append(me & (bit ^ core) != 0)
        parity = parity ^ upper[-1]
    upper.append(parity)
    genes, samples = expression.shape
    place = jnp.broadcast_to(mine, (TILE, genes))
    scales = jnp.broadcast_to(
        (powers.astype(jnp.float32) * LOG2E)[:, None, None], (npower, TILE, genes)
    )

    width = samples // PIECES
    pieces = tuple(expression[:, i * width : (i + 1) * width] for i in range(PIECES))
    lane_blocks = [(expression,)]
    for i, bit in enumerate(far):
        sent = [pieces] if i == 0 else lane_blocks
        lane_blocks = lane_blocks + [
            tuple(from_partner(part, bit) for part in parts)
            for parts in sent
        ]
    sub_blocks = [expression]
    for bit in near:
        sub_blocks += [from_partner(block, bit) for block in sub_blocks]
    crossed = [from_partner(block, core) for block in sub_blocks]

    quarter = max(len(lane_blocks) // 4, 1)
    here, last = lane_blocks[:-quarter], lane_blocks[-quarter:]
    quarter = max(len(sub_blocks) // 4, 1)
    first = sub_blocks[:-quarter] + crossed[:-quarter]
    second = sub_blocks[-quarter:] + crossed[-quarter:]
    part, first_stats = early_sums(scales, place, here, first)
    part = late_sums(scales, place, here, last, first, second, first_stats, part)

    for bit in far:
        part = part + from_partner(part, bit)
    own, part = part, part[None]
    for bit, up in zip(near + [core], upper):
        got = from_partner(part, bit)
        part = jnp.concatenate([jnp.where(up, got, part), jnp.where(up, part, got)])

    log_degree, degree_freq, fit_slope, mean_log = fit(npower, len(lane_blocks), place, part, own)
    return log_degree, degree_freq, fit_slope[0], mean_log[0]


def solution(mesh):
    return jax.shard_map(
        on_device,
        mesh=mesh,
        in_specs=(P(AXES, None), P()),
        out_specs=(P(None, AXES), P(), P(), P()),
        check_vma=False,
    )
```

```python
import functools

import jax
import jax.numpy as jnp
from jax import lax
from jax.experimental import pallas as pl
from jax.experimental.pallas import tpu as pltpu
from jax.sharding import PartitionSpec as P


BINS = 10
AXES = ("row", "col")
LOG2E = 1.4426950408889634
LOG10E = 0.4342944819032518
TILE = 8
CHUNK = 32
PIECES = 2
VMEM_LIMIT = 20 * 2**20


def gene_stats(genes):
    values = genes.astype(jnp.float32)
    samples = values.shape[1]
    mean = jnp.sum(values, axis=1, keepdims=True) * (1.0 / samples)
    centred = values - mean
    var = jnp.sum(centred * centred, axis=1, keepdims=True) * (1.0 / samples)
    return mean, lax.rsqrt(var + 1e-06)


def as_row(column):
    genes = column.shape[0]
    return jnp.transpose(jnp.broadcast_to(column, (genes, genes)))[0:1, :]


def vmem_spec():
    return pl.BlockSpec(memory_space=pltpu.VMEM)


def pallas(kernel, out_shape, operands, scratch=(), cost=None, scalars=0):
    return pl.pallas_call(
        kernel,
        out_shape=out_shape,
        in_specs=[pl.BlockSpec(memory_space=pltpu.SMEM)] * scalars
        + [vmem_spec()] * (len(operands) - scalars),
        out_specs=jax.tree.map(lambda _: vmem_spec(), out_shape),
        scratch_shapes=list(scratch),
        compiler_params=pltpu.CompilerParams(vmem_limit_bytes=VMEM_LIMIT),
        cost_estimate=cost,
    )(*operands)


def f32(*shape):
    return jax.ShapeDtypeStruct(shape, jnp.float32)


def split_refs(refs, sizes):
    groups = []
    for size in sizes:
        groups.append(refs[:size])
        refs = refs[size:]
    return groups, refs


def whole(parts):
    return jnp.concatenate([part[...] for part in parts], axis=1)


def measure_sub(block, out):
    genes, samples = block.shape
    mean, inv = gene_stats(block)
    out[0] = jnp.broadcast_to(mean * samples, (genes, genes))
    out[1] = jnp.broadcast_to(inv * (1.0 / samples), (genes, genes))


def row_sums(raw, column, sub_stats, lane_mean, lane_inv, scales):
    npower, _, genes = scales.shape
    sums = [jnp.zeros((TILE, genes), jnp.float32) for _ in range(npower)]
    for b, stat in enumerate(sub_stats):
        for c in range(0, genes, CHUNK):
            part = slice(c, c + CHUNK)
            pearson = (
                (raw[b, part, column] - stat[0, part, :] * lane_mean)
                * stat[1, part, :]
                * lane_inv
            )
            log_abs = jnp.log(jnp.abs(pearson)).reshape(CHUNK // TILE, TILE, genes)
            for p in range(npower):
                term = jnp.exp2(log_abs * scales[p])
                sums[p] = sums[p] + jnp.sum(term, axis=0)
    return [jnp.sum(total, axis=0, keepdims=True) for total in sums]


def multiply(raw, sub_refs, lanes):
    for b, sub_ref in enumerate(sub_refs):
        raw[b] = lax.dot_general(
            sub_ref[...], lanes, (((1,), (1,)), ((), ())), preferred_element_type=jnp.float32
        )


def first_kernel(sub_count, powers, lane, *refs):
    subs, (scales, out, sub_stats, raw) = refs[:sub_count], refs[sub_count:]
    npower, tile, genes = scales.shape
    for p in range(npower):
        scales[p] = jnp.full((tile, genes), powers[p].astype(jnp.float32) * LOG2E)
    block = lane[...]
    multiply(raw, subs, block)
    for b, sub in enumerate(subs):
        measure_sub(sub[...], sub_stats.at[b])
    mean, inv = gene_stats(block)
    mean, inv = as_row(mean), as_row(inv)
    stat_refs = [sub_stats.at[b] for b in range(sub_count)]
    rows = row_sums(raw, slice(0, genes), stat_refs, mean, inv, scales)
    for p, row in enumerate(rows + [mean, inv]):
        out[0, p : p + 1, :] = row


def early_kernel(lane_sizes, known_count, new_count, scales, place, *refs):
    lanes, refs = split_refs(refs, lane_sizes)
    (known, new), refs = split_refs(refs, (known_count, new_count))
    stat_refs = []
    if known_count:
        stat_refs, refs = [refs[0].at[b] for b in range(known_count)], refs[1:]
    prior, out, new_stats, raw = refs
    npower, _, genes = scales.shape
    blocks = [whole(parts) for parts in lanes]
    multiply(raw, new + known, jnp.concatenate(blocks, axis=0))
    for b, sub in enumerate(new):
        measure_sub(sub[...], new_stats.at[b])
    new_refs = [new_stats.at[b] for b in range(new_count)]
    for a, block in enumerate(blocks):
        column = slice(a * genes, (a + 1) * genes)
        if a < prior.shape[0]:
            begun = [prior[a, p : p + 1, :] for p in range(npower + 2)]
            mean, inv = begun[npower:]
            rows = row_sums(raw, column, new_refs, mean, inv, scales)
            rows = [row + begun[p] for p, row in enumerate(rows)]
        else:
            mean, inv = gene_stats(block)
            mean, inv = as_row(mean), as_row(inv)
            rows = row_sums(raw, column, new_refs + stat_refs, mean, inv, scales)
        for p, row in enumerate(rows + [mean, inv]):
            out[a, p : p + 1, :] = row


def late_kernel(here_sizes, last_sizes, counts, second_count, scales, place, *refs):
    here, refs = split_refs(refs, here_sizes)
    last, refs = split_refs(refs, last_sizes)
    (first, second), refs = split_refs(refs, (sum(counts), second_count))
    stat_arrays, refs = refs[: len(counts)], refs[len(counts) :]
    prior, out, raw_here, raw_last, second_stats = refs
    npower, _, genes = scales.shape
    slots = len(here) + len(last)
    full, rest = npower // TILE, npower % TILE
    second_refs = [second_stats.at[b] for b in range(second_count)]
    all_refs = [ref.at[b] for ref, count in zip(stat_arrays, counts) for b in range(count)]
    all_refs += second_refs
    rows = []
    multiply(raw_here, second, jnp.concatenate([whole(parts) for parts in here], axis=0))
    for b, sub in enumerate(second):
        measure_sub(sub[...], second_stats.at[b])
    blocks = [whole(parts) for parts in last]
    multiply(raw_last, first + second, jnp.concatenate(blocks, axis=0))
    for a in range(len(here)):
        mean, inv = prior[a, npower : npower + 1, :], prior[a, npower + 1 : npower + 2, :]
        column = slice(a * genes, (a + 1) * genes)
        added = row_sums(raw_here, column, second_refs, mean, inv, scales)
        rows.append([row + prior[a, p : p + 1, :] for p, row in enumerate(added)])
    for a, block in enumerate(blocks):
        mean, inv = gene_stats(block)
        column = slice(a * genes, (a + 1) * genes)
        rows.append(row_sums(raw_last, column, all_refs, as_row(mean), as_row(inv), scales))

    mine = place[...]
    sublane = lax.broadcasted_iota(jnp.int32, (TILE, genes), 0)
    for f in range(full):
        for target in range(slots):
            tile = jnp.concatenate(rows[0][f * TILE : (f + 1) * TILE], axis=0)
            for s in range(1, slots):
                other = jnp.concatenate(rows[s][f * TILE : (f + 1) * TILE], axis=0)
                tile = jnp.where(mine == (s ^ target), other, tile)
            out[f * slots + target] = tile
    for t in range(out.shape[0] - full * slots):
        tile = jnp.zeros((TILE, genes), jnp.float32)
        for q in range(rest):
            for s in range(slots):
                hit = sublane + t * TILE == q * slots + (mine ^ s)
                tile = jnp.where(hit, rows[s][full * TILE + q], tile)
        out[full * slots + t] = tile


def tile_count(npower, slots):
    return slots * (npower // TILE) + -(-(npower % TILE) * slots // TILE)


def work(pairs, samples, npower):
    return pl.CostEstimate(
        flops=2 * pairs * samples, bytes_accessed=4 * pairs, transcendentals=pairs * (npower + 1)
    )


def flat(blocks):
    return [part for parts in blocks for part in parts]


def sizes_of(blocks):
    return [len(parts) for parts in blocks]


def first_sums(powers, lane, subs):
    genes, samples = lane.shape
    npower = powers.shape[0]
    return pallas(
        functools.partial(first_kernel, len(subs)),
        (
            f32(npower, TILE, genes),
            f32(1, npower + 2, genes),
            f32(len(subs), 2, genes, genes),
        ),
        [powers, lane] + subs,
        [pltpu.VMEM((len(subs), genes, genes), jnp.float32)],
        work(len(subs) * genes * genes, samples, npower),
        scalars=1,
    )


def early_sums(scales, place, here, known, new, known_stats, prior):
    genes, samples = new[0].shape
    npower = scales.shape[0]
    count = len(known) + len(new)
    return pallas(
        functools.partial(early_kernel, sizes_of(here), len(known), len(new)),
        (f32(len(here), npower + 2, genes), f32(len(new), 2, genes, genes)),
        [scales, place] + flat(here) + known + new + known_stats + [prior],
        [pltpu.VMEM((count, genes, len(here) * genes), jnp.float32)],
        work(len(here) * count * genes * genes, samples, npower),
    )


def late_sums(scales, place, here, last, first, second, first_stats, prior):
    genes, samples = first[0].shape
    npower = scales.shape[0]
    blocks = len(here) * len(second) + len(last) * (len(first) + len(second))
    return pallas(
        functools.partial(
            late_kernel,
            sizes_of(here),
            sizes_of(last),
            [array.shape[0] for array in first_stats],
            len(second),
        ),
        f32(tile_count(npower, len(here) + len(last)), TILE, genes),
        [scales, place] + flat(here) + flat(last) + first + second + first_stats + [prior],
        [
            pltpu.VMEM((len(second), genes, len(here) * genes), jnp.float32),
            pltpu.VMEM((len(first) + len(second), genes, len(last) * genes), jnp.float32),
            pltpu.VMEM((len(second), 2, genes, genes), jnp.float32),
        ],
        work(blocks * genes * genes, samples, npower),
    )


def fit_kernel(npower, slots, place, deg, own, log_degree, degree_freq, fit_slope, mean_log):
    groups, tiles, _, genes = deg.shape
    full, rest = npower // TILE, npower % TILE
    total_genes = groups * slots * genes
    inv_genes = 1.0 / total_genes
    mine = place[...]
    tail = tiles - slots * full
    sublane = lax.broadcasted_iota(jnp.int32, (TILE, genes), 0)
    lane = lax.broadcasted_iota(jnp.int32, (TILE, genes), 1)
    slope_row, mean_row = 0.0, 0.0

    def hat(value, inverse, counts):
        position = jnp.clip(BINS * value * inverse - 0.5, 0.0, BINS - 1.0)
        return [
            count + jnp.maximum(0.0, 1.0 - jnp.abs(position - b)) for b, count in enumerate(counts)
        ]

    def line(peak, freq, total):
        used = lane < BINS
        centre = lane.astype(jnp.float32) + 0.5
        xfit = jnp.where(used, jnp.log(centre * peak * (1.0 / BINS)) * LOG10E, 0.0)
        yfit = jnp.where(used, jnp.log(freq + inv_genes) * LOG10E, 0.0)
        xdev = jnp.where(used, xfit - jnp.sum(xfit, axis=1, keepdims=True) * (1.0 / BINS), 0.0)
        ydev = jnp.where(used, yfit - jnp.sum(yfit, axis=1, keepdims=True) * (1.0 / BINS), 0.0)
        slope = jnp.sum(xdev * ydev, axis=1, keepdims=True) / jnp.sum(
            xdev * xdev, axis=1, keepdims=True
        )
        return slope, jnp.log(total * inv_genes) * LOG10E

    def on_lanes(counts):
        freq = jnp.zeros((TILE, genes), jnp.float32)
        for b in range(BINS):
            freq = jnp.where(lane == b, counts[b] * inv_genes, freq)
        return freq

    zero = jnp.zeros((TILE, genes), jnp.float32)
    for f in range(full):
        top = deg[0, f * slots]
        for g in range(groups):
            for s in range(slots):
                top = jnp.maximum(top, deg[g, f * slots + s])
        peak = jnp.max(top, axis=1, keepdims=True)
        inverse = 1.0 / peak
        total, counts = zero, [zero] * BINS
        for g in range(groups):
            for s in range(slots):
                value = deg[g, f * slots + s]
                total = total + value
                counts = hat(value, inverse, counts)
        freq = on_lanes([jnp.sum(count, axis=1, keepdims=True) for count in counts])
        slope, mean = line(peak, freq, jnp.sum(total, axis=1, keepdims=True))
        value = own[f * slots]
        for s in range(1, slots):
            value = jnp.where(mine == s, own[f * slots + s], value)
        log_degree[f * TILE : (f + 1) * TILE, :] = jnp.log(value) * LOG10E
        degree_freq[f * TILE : (f + 1) * TILE, :] = freq[:, :BINS]
        diagonal = lane == sublane + f * TILE
        slope_row += jnp.sum(jnp.where(diagonal, slope, 0.0), axis=0, keepdims=True)
        mean_row += jnp.sum(jnp.where(diagonal, mean, 0.0), axis=0, keepdims=True)

    if rest:
        base = slots * full
        row_power = [(sublane + t * TILE) // slots for t in range(tail)]
        row_slot = [(sublane + t * TILE) % slots for t in range(tail)]

        def per_power(columns, combine, neutral):
            whole = [zero for _ in range(tail)]
            for q in range(rest):
                picked = [
                    jnp.where(row_power[t] == q, columns[t], neutral) for t in range(tail)
                ]
                merged = functools.reduce(combine, picked)
                reduce = jnp.max if combine is jnp.maximum else jnp.sum
                value = reduce(merged, axis=0, keepdims=True)
                whole = [jnp.where(row_power[t] == q, value, whole[t]) for t in range(tail)]
            return whole

        tops, totals, counts = [], [], []
        for t in range(tail):
            top = deg[0, base + t]
            for g in range(groups):
                top = jnp.maximum(top, deg[g, base + t])
            tops.append(jnp.max(top, axis=1, keepdims=True))
        peaks = per_power(tops, jnp.maximum, 0.0)
        for t in range(tail):
            inverse = 1.0 / peaks[t]
            total, count = zero, [zero] * BINS
            for g in range(groups):
                value = deg[g, base + t]
                total = total + value
                count = hat(value, inverse, count)
            totals.append(jnp.sum(total, axis=1, keepdims=True))
            counts.append([jnp.sum(c, axis=1, keepdims=True) for c in count])
        totals = per_power(totals, jnp.add, 0.0)
        freqs = per_power([on_lanes(c) for c in counts], jnp.add, 0.0)
        for q in range(rest):
            t, r = q * slots // TILE, q * slots % TILE
            p = full * TILE + q
            slope, mean = line(peaks[t], freqs[t], totals[t])
            degree_freq[p : p + 1, :] = freqs[t][r : r + 1, :BINS]
            here = (lane == p) & (sublane == r)
            slope_row += jnp.sum(jnp.where(here, slope, 0.0), axis=0, keepdims=True)
            mean_row += jnp.sum(jnp.where(here, mean, 0.0), axis=0, keepdims=True)
            value = zero
            for t in range(tail):
                hit = (row_power[t] == q) & (row_slot[t] == mine)
                value = value + jnp.where(hit, own[base + t], 0.0)
            log_degree[p : p + 1, :] = jnp.log(jnp.sum(value, axis=0, keepdims=True)) * LOG10E
    fit_slope[...] = slope_row[:, :npower]
    mean_log[...] = mean_row[:, :npower]


def fit(npower, slots, place, deg, own):
    genes = deg.shape[-1]
    return pallas(
        functools.partial(fit_kernel, npower, slots),
        (f32(npower, genes), f32(npower, BINS), f32(1, npower), f32(1, npower)),
        [place, deg, own],
    )


def bits_of(low, high):
    bits = []
    while low < high:
        bits.append(low)
        low *= 2
    return bits


def split_bits(rows, cols):
    devices = rows * cols
    col_bits, row_bits = bits_of(1, cols), bits_of(2 * cols, devices)
    far = col_bits[len(col_bits) // 2 :] + row_bits[len(row_bits) // 2 :]
    near = col_bits[: len(col_bits) // 2] + row_bits[: len(row_bits) // 2]
    return [bit ^ cols for bit in far], [bit ^ cols for bit in near]


def on_device(expression, powers):
    rows, cols = lax.axis_size("row"), lax.axis_size("col")
    devices = rows * cols
    npower = powers.shape[0]
    me = lax.axis_index(AXES)
    far, near = split_bits(rows, cols)
    core = cols

    def from_partner(array, bit):
        return lax.ppermute(array, AXES, [(i, i ^ bit) for i in range(devices)])

    mine = jnp.zeros((), jnp.int32)
    parity = me & core != 0
    for i, bit in enumerate(far):
        mine = mine | jnp.where(me & (bit ^ core) != 0, 1 << i, 0)
        parity = parity ^ (me & (bit ^ core) != 0)
    upper = []
    for bit in near:
        upper.append(me & (bit ^ core) != 0)
        parity = parity ^ upper[-1]
    upper.append(parity)
    genes, samples = expression.shape
    place = jnp.broadcast_to(mine, (TILE, genes))

    width = samples // PIECES
    pieces = tuple(expression[:, i * width : (i + 1) * width] for i in range(PIECES))
    lane_blocks = [(expression,)]
    for i, bit in enumerate(far):
        sent = [pieces] if i == 0 else lane_blocks
        lane_blocks = lane_blocks + [
            tuple(from_partner(part, bit) for part in parts)
            for parts in sent
        ]
    sub_blocks = [expression]
    for bit in near:
        sub_blocks += [from_partner(block, bit) for block in sub_blocks]
    crossed = [from_partner(block, core) for block in sub_blocks]

    quarter = max(len(lane_blocks) // 4, 1)
    here, last = lane_blocks[:-quarter], lane_blocks[-quarter:]
    quarter = max(len(sub_blocks) // 4, 1)
    known = [sub_blocks[0], crossed[0]]
    new = sub_blocks[1:-quarter] + crossed[1:-quarter]
    second, third = sub_blocks[-quarter:], crossed[-quarter:]
    scales, part, stats = first_sums(powers, expression, known)
    stats = [stats]
    part, new_stats = early_sums(scales, place, here, known, new, stats, part)
    stats.append(new_stats)
    part, new_stats = early_sums(scales, place, here, [], second, [], part)
    stats.append(new_stats)
    ready = known + new + second
    part = late_sums(scales, place, here, last, ready, third, stats, part)

    for bit in far:
        part = part + from_partner(part, bit)
    own, part = part, part[None]
    for bit, up in zip(near + [core], upper):
        got = from_partner(part, bit)
        part = jnp.concatenate([jnp.where(up, got, part), jnp.where(up, part, got)])

    log_degree, degree_freq, fit_slope, mean_log = fit(npower, len(lane_blocks), place, part, own)
    return log_degree, degree_freq, fit_slope[0], mean_log[0]


def solution(mesh):
    return jax.shard_map(
        on_device,
        mesh=mesh,
        in_specs=(P(AXES, None), P()),
        out_specs=(P(None, AXES), P(), P(), P()),
        check_vma=False,
    )
```

```python
import functools

import jax
import jax.numpy as jnp
from jax import lax
from jax.experimental import pallas as pl
from jax.experimental.pallas import tpu as pltpu
from jax.sharding import PartitionSpec as P


BINS = 10
AXES = ("row", "col")
LOG2E = 1.4426950408889634
LOG10E = 0.4342944819032518
TILE = 8
CHUNK = 32
PIECES = 2
VMEM_LIMIT = 20 * 2**20


def gene_stats(genes):
    values = genes.astype(jnp.float32)
    samples = values.shape[1]
    mean = jnp.sum(values, axis=1, keepdims=True) * (1.0 / samples)
    centred = values - mean
    var = jnp.sum(centred * centred, axis=1, keepdims=True) * (1.0 / samples)
    return mean, lax.rsqrt(var + 1e-06)


def as_row(column):
    genes = column.shape[0]
    return jnp.transpose(jnp.broadcast_to(column, (genes, genes)))[0:1, :]


def vmem_spec():
    return pl.BlockSpec(memory_space=pltpu.VMEM)


def pallas(kernel, out_shape, operands, scratch=(), cost=None, scalars=0):
    return pl.pallas_call(
        kernel,
        out_shape=out_shape,
        in_specs=[pl.BlockSpec(memory_space=pltpu.SMEM)] * scalars
        + [vmem_spec()] * (len(operands) - scalars),
        out_specs=jax.tree.map(lambda _: vmem_spec(), out_shape),
        scratch_shapes=list(scratch),
        compiler_params=pltpu.CompilerParams(vmem_limit_bytes=VMEM_LIMIT),
        cost_estimate=cost,
    )(*operands)


def f32(*shape):
    return jax.ShapeDtypeStruct(shape, jnp.float32)


def split_refs(refs, sizes):
    groups = []
    for size in sizes:
        groups.append(refs[:size])
        refs = refs[size:]
    return groups, refs


def whole(parts):
    return jnp.concatenate([part[...] for part in parts], axis=1)


def measure_sub(block, out):
    genes, samples = block.shape
    mean, inv = gene_stats(block)
    out[0] = jnp.broadcast_to(mean * samples, (genes, genes))
    out[1] = jnp.broadcast_to(inv * (1.0 / samples), (genes, genes))


def row_sums(raw, column, sub_stats, lane_mean, lane_inv, scales):
    npower, _, genes = scales.shape
    sums = [jnp.zeros((TILE, genes), jnp.float32) for _ in range(npower)]
    for b, stat in enumerate(sub_stats):
        for c in range(0, genes, CHUNK):
            part = slice(c, c + CHUNK)
            pearson = (
                (raw[b, part, column] - stat[0, part, :] * lane_mean)
                * stat[1, part, :]
                * lane_inv
            )
            log_abs = jnp.log(jnp.abs(pearson)).reshape(CHUNK // TILE, TILE, genes)
            for p in range(npower):
                term = jnp.exp2(log_abs * scales[p])
                sums[p] = sums[p] + jnp.sum(term, axis=0)
    return [jnp.sum(total, axis=0, keepdims=True) for total in sums]


def multiply(raw, sub_refs, lanes):
    for b, sub_ref in enumerate(sub_refs):
        raw[b] = lax.dot_general(
            sub_ref[...], lanes, (((1,), (1,)), ((), ())), preferred_element_type=jnp.float32
        )


def first_kernel(sub_count, powers, lane, *refs):
    subs, (scales, out, sub_stats, raw) = refs[:sub_count], refs[sub_count:]
    npower, tile, genes = scales.shape
    for p in range(npower):
        scales[p] = jnp.full((tile, genes), powers[p].astype(jnp.float32) * LOG2E)
    block = lane[...]
    multiply(raw, subs, block)
    for b, sub in enumerate(subs):
        measure_sub(sub[...], sub_stats.at[b])
    mean, inv = gene_stats(block)
    mean, inv = as_row(mean), as_row(inv)
    stat_refs = [sub_stats.at[b] for b in range(sub_count)]
    rows = row_sums(raw, slice(0, genes), stat_refs, mean, inv, scales)
    for p, row in enumerate(rows + [mean, inv]):
        out[0, p : p + 1, :] = row


def early_kernel(lane_sizes, known_count, new_count, scales, place, *refs):
    lanes, refs = split_refs(refs, lane_sizes)
    (known, new), refs = split_refs(refs, (known_count, new_count))
    stat_refs = []
    if known_count:
        stat_refs, refs = [refs[0].at[b] for b in range(known_count)], refs[1:]
    prior, out, new_stats, raw = refs
    npower, _, genes = scales.shape
    blocks = [whole(parts) for parts in lanes]
    multiply(raw, new + known, jnp.concatenate(blocks, axis=0))
    for b, sub in enumerate(new):
        measure_sub(sub[...], new_stats.at[b])
    new_refs = [new_stats.at[b] for b in range(new_count)]
    for a, block in enumerate(blocks):
        column = slice(a * genes, (a + 1) * genes)
        if a < prior.shape[0]:
            begun = [prior[a, p : p + 1, :] for p in range(npower + 2)]
            mean, inv = begun[npower:]
            rows = row_sums(raw, column, new_refs, mean, inv, scales)
            rows = [row + begun[p] for p, row in enumerate(rows)]
        else:
            mean, inv = gene_stats(block)
            mean, inv = as_row(mean), as_row(inv)
            rows = row_sums(raw, column, new_refs + stat_refs, mean, inv, scales)
        for p, row in enumerate(rows + [mean, inv]):
            out[a, p : p + 1, :] = row


def late_kernel(here_sizes, last_sizes, counts, second_count, scales, place, *refs):
    here, refs = split_refs(refs, here_sizes)
    last, refs = split_refs(refs, last_sizes)
    (first, second), refs = split_refs(refs, (sum(counts), second_count))
    stat_arrays, refs = refs[: len(counts)], refs[len(counts) :]
    prior, out, raw_here, raw_last, second_stats = refs
    npower, _, genes = scales.shape
    slots = len(here) + len(last)
    full, rest = npower // TILE, npower % TILE
    second_refs = [second_stats.at[b] for b in range(second_count)]
    all_refs = [ref.at[b] for ref, count in zip(stat_arrays, counts) for b in range(count)]
    all_refs += second_refs
    rows = []
    multiply(raw_here, second, jnp.concatenate([whole(parts) for parts in here], axis=0))
    for b, sub in enumerate(second):
        measure_sub(sub[...], second_stats.at[b])
    blocks = [whole(parts) for parts in last]
    multiply(raw_last, first + second, jnp.concatenate(blocks, axis=0))
    for a in range(len(here)):
        mean, inv = prior[a, npower : npower + 1, :], prior[a, npower + 1 : npower + 2, :]
        column = slice(a * genes, (a + 1) * genes)
        added = row_sums(raw_here, column, second_refs, mean, inv, scales)
        rows.append([row + prior[a, p : p + 1, :] for p, row in enumerate(added)])
    for a, block in enumerate(blocks):
        mean, inv = gene_stats(block)
        column = slice(a * genes, (a + 1) * genes)
        rows.append(row_sums(raw_last, column, all_refs, as_row(mean), as_row(inv), scales))

    mine = place[...]
    sublane = lax.broadcasted_iota(jnp.int32, (TILE, genes), 0)
    for f in range(full):
        for target in range(slots):
            tile = jnp.concatenate(rows[0][f * TILE : (f + 1) * TILE], axis=0)
            for s in range(1, slots):
                other = jnp.concatenate(rows[s][f * TILE : (f + 1) * TILE], axis=0)
                tile = jnp.where(mine == (s ^ target), other, tile)
            out[f * slots + target] = tile
    for t in range(out.shape[0] - full * slots):
        tile = jnp.zeros((TILE, genes), jnp.float32)
        for q in range(rest):
            for s in range(slots):
                hit = sublane + t * TILE == q * slots + (mine ^ s)
                tile = jnp.where(hit, rows[s][full * TILE + q], tile)
        out[full * slots + t] = tile


def tile_count(npower, slots):
    return slots * (npower // TILE) + -(-(npower % TILE) * slots // TILE)


def work(pairs, samples, npower):
    return pl.CostEstimate(
        flops=2 * pairs * samples, bytes_accessed=4 * pairs, transcendentals=pairs * (npower + 1)
    )


def flat(blocks):
    return [part for parts in blocks for part in parts]


def sizes_of(blocks):
    return [len(parts) for parts in blocks]


def first_sums(powers, lane, subs):
    genes, samples = lane.shape
    npower = powers.shape[0]
    return pallas(
        functools.partial(first_kernel, len(subs)),
        (
            f32(npower, TILE, genes),
            f32(1, npower + 2, genes),
            f32(len(subs), 2, genes, genes),
        ),
        [powers, lane] + subs,
        [pltpu.VMEM((len(subs), genes, genes), jnp.float32)],
        work(len(subs) * genes * genes, samples, npower),
        scalars=1,
    )


def early_sums(scales, place, here, known, new, known_stats, prior):
    genes, samples = new[0].shape
    npower = scales.shape[0]
    count = len(known) + len(new)
    return pallas(
        functools.partial(early_kernel, sizes_of(here), len(known), len(new)),
        (f32(len(here), npower + 2, genes), f32(len(new), 2, genes, genes)),
        [scales, place] + flat(here) + known + new + known_stats + [prior],
        [pltpu.VMEM((count, genes, len(here) * genes), jnp.float32)],
        work(len(here) * count * genes * genes, samples, npower),
    )


def late_sums(scales, place, here, last, first, second, first_stats, prior):
    genes, samples = first[0].shape
    npower = scales.shape[0]
    blocks = len(here) * len(second) + len(last) * (len(first) + len(second))
    return pallas(
        functools.partial(
            late_kernel,
            sizes_of(here),
            sizes_of(last),
            [array.shape[0] for array in first_stats],
            len(second),
        ),
        f32(tile_count(npower, len(here) + len(last)), TILE, genes),
        [scales, place] + flat(here) + flat(last) + first + second + first_stats + [prior],
        [
            pltpu.VMEM((len(second), genes, len(here) * genes), jnp.float32),
            pltpu.VMEM((len(first) + len(second), genes, len(last) * genes), jnp.float32),
            pltpu.VMEM((len(second), 2, genes, genes), jnp.float32),
        ],
        work(blocks * genes * genes, samples, npower),
    )


def fit_kernel(npower, slots, place, deg, own, log_degree, degree_freq, fit_slope, mean_log):
    groups, tiles, _, genes = deg.shape
    full, rest = npower // TILE, npower % TILE
    total_genes = groups * slots * genes
    inv_genes = 1.0 / total_genes
    mine = place[...]
    tail = tiles - slots * full
    sublane = lax.broadcasted_iota(jnp.int32, (TILE, genes), 0)
    lane = lax.broadcasted_iota(jnp.int32, (TILE, genes), 1)
    slope_row, mean_row = 0.0, 0.0

    def hat(value, inverse, counts):
        position = jnp.clip(BINS * value * inverse - 0.5, 0.0, BINS - 1.0)
        return [
            count + jnp.maximum(0.0, 1.0 - jnp.abs(position - b)) for b, count in enumerate(counts)
        ]

    def line(peak, freq, total):
        used = lane < BINS
        centre = lane.astype(jnp.float32) + 0.5
        xfit = jnp.where(used, jnp.log(centre * peak * (1.0 / BINS)) * LOG10E, 0.0)
        yfit = jnp.where(used, jnp.log(freq + inv_genes) * LOG10E, 0.0)
        xdev = jnp.where(used, xfit - jnp.sum(xfit, axis=1, keepdims=True) * (1.0 / BINS), 0.0)
        ydev = jnp.where(used, yfit - jnp.sum(yfit, axis=1, keepdims=True) * (1.0 / BINS), 0.0)
        slope = jnp.sum(xdev * ydev, axis=1, keepdims=True) / jnp.sum(
            xdev * xdev, axis=1, keepdims=True
        )
        return slope, jnp.log(total * inv_genes) * LOG10E

    def on_lanes(counts):
        freq = jnp.zeros((TILE, genes), jnp.float32)
        for b in range(BINS):
            freq = jnp.where(lane == b, counts[b] * inv_genes, freq)
        return freq

    zero = jnp.zeros((TILE, genes), jnp.float32)
    for f in range(full):
        top = deg[0, f * slots]
        for g in range(groups):
            for s in range(slots):
                top = jnp.maximum(top, deg[g, f * slots + s])
        peak = jnp.max(top, axis=1, keepdims=True)
        inverse = 1.0 / peak
        total, counts = zero, [zero] * BINS
        for g in range(groups):
            for s in range(slots):
                value = deg[g, f * slots + s]
                total = total + value
                counts = hat(value, inverse, counts)
        freq = on_lanes([jnp.sum(count, axis=1, keepdims=True) for count in counts])
        slope, mean = line(peak, freq, jnp.sum(total, axis=1, keepdims=True))
        value = own[f * slots]
        for s in range(1, slots):
            value = jnp.where(mine == s, own[f * slots + s], value)
        log_degree[f * TILE : (f + 1) * TILE, :] = jnp.log(value) * LOG10E
        degree_freq[f * TILE : (f + 1) * TILE, :] = freq[:, :BINS]
        diagonal = lane == sublane + f * TILE
        slope_row += jnp.sum(jnp.where(diagonal, slope, 0.0), axis=0, keepdims=True)
        mean_row += jnp.sum(jnp.where(diagonal, mean, 0.0), axis=0, keepdims=True)

    if rest:
        base = slots * full
        row_power = [(sublane + t * TILE) // slots for t in range(tail)]
        row_slot = [(sublane + t * TILE) % slots for t in range(tail)]

        def per_power(columns, combine, neutral):
            whole = [zero for _ in range(tail)]
            for q in range(rest):
                picked = [
                    jnp.where(row_power[t] == q, columns[t], neutral) for t in range(tail)
                ]
                merged = functools.reduce(combine, picked)
                reduce = jnp.max if combine is jnp.maximum else jnp.sum
                value = reduce(merged, axis=0, keepdims=True)
                whole = [jnp.where(row_power[t] == q, value, whole[t]) for t in range(tail)]
            return whole

        tops, totals, counts = [], [], []
        for t in range(tail):
            top = deg[0, base + t]
            for g in range(groups):
                top = jnp.maximum(top, deg[g, base + t])
            tops.append(jnp.max(top, axis=1, keepdims=True))
        peaks = per_power(tops, jnp.maximum, 0.0)
        for t in range(tail):
            inverse = 1.0 / peaks[t]
            total, count = zero, [zero] * BINS
            for g in range(groups):
                value = deg[g, base + t]
                total = total + value
                count = hat(value, inverse, count)
            totals.append(jnp.sum(total, axis=1, keepdims=True))
            counts.append([jnp.sum(c, axis=1, keepdims=True) for c in count])
        totals = per_power(totals, jnp.add, 0.0)
        freqs = per_power([on_lanes(c) for c in counts], jnp.add, 0.0)
        for q in range(rest):
            t, r = q * slots // TILE, q * slots % TILE
            p = full * TILE + q
            slope, mean = line(peaks[t], freqs[t], totals[t])
            degree_freq[p : p + 1, :] = freqs[t][r : r + 1, :BINS]
            here = (lane == p) & (sublane == r)
            slope_row += jnp.sum(jnp.where(here, slope, 0.0), axis=0, keepdims=True)
            mean_row += jnp.sum(jnp.where(here, mean, 0.0), axis=0, keepdims=True)
            value = zero
            for t in range(tail):
                hit = (row_power[t] == q) & (row_slot[t] == mine)
                value = value + jnp.where(hit, own[base + t], 0.0)
            log_degree[p : p + 1, :] = jnp.log(jnp.sum(value, axis=0, keepdims=True)) * LOG10E
    fit_slope[...] = slope_row[:, :npower]
    mean_log[...] = mean_row[:, :npower]


def fit(npower, slots, place, deg, own):
    genes = deg.shape[-1]
    return pallas(
        functools.partial(fit_kernel, npower, slots),
        (f32(npower, genes), f32(npower, BINS), f32(1, npower), f32(1, npower)),
        [place, deg, own],
    )


def bits_of(low, high):
    bits = []
    while low < high:
        bits.append(low)
        low *= 2
    return bits


def split_bits(rows, cols):
    devices = rows * cols
    col_bits, row_bits = bits_of(1, cols), bits_of(2 * cols, devices)
    far = col_bits[len(col_bits) // 2 :] + row_bits[len(row_bits) // 2 :]
    near = col_bits[: len(col_bits) // 2] + row_bits[: len(row_bits) // 2]
    return [bit ^ cols for bit in far], [bit ^ cols for bit in near]


def span(bits):
    masks = [0]
    for bit in bits:
        masks += [mask ^ bit for mask in masks]
    return masks


def on_device(expression, powers):
    rows, cols = lax.axis_size("row"), lax.axis_size("col")
    devices = rows * cols
    npower = powers.shape[0]
    me = lax.axis_index(AXES)
    far, near = split_bits(rows, cols)
    core = cols

    def from_partner(array, bit):
        return lax.ppermute(array, AXES, [(i, i ^ bit) for i in range(devices)])

    mine = jnp.zeros((), jnp.int32)
    parity = me & core != 0
    for i, bit in enumerate(far):
        mine = mine | jnp.where(me & (bit ^ core) != 0, 1 << i, 0)
        parity = parity ^ (me & (bit ^ core) != 0)
    upper = []
    for bit in near:
        upper.append(me & (bit ^ core) != 0)
        parity = parity ^ upper[-1]
    upper.append(parity)
    genes, samples = expression.shape
    place = jnp.broadcast_to(mine, (TILE, genes))

    width = samples // PIECES
    pieces, source = [], expression
    for i in range(PIECES):
        pieces.append(source[:, i * width : (i + 1) * width])
        source = lax.optimization_barrier(source)
    lane_blocks = [(expression,)]
    for i, bit in enumerate(far):
        sent = [pieces] if i == 0 else lane_blocks
        lane_blocks = lane_blocks + [
            tuple(from_partner(part, bit) for part in parts)
            for parts in sent
        ]
    sub_blocks = [expression]
    for bit in near:
        sub_blocks += [from_partner(block, bit) for block in sub_blocks]
    crossed = [from_partner(block, core) for block in sub_blocks]

    quarter = max(len(lane_blocks) // 4, 1)
    here, last = lane_blocks[:-quarter], lane_blocks[-quarter:]
    quarter = max(len(sub_blocks) // 4, 1)
    known = [sub_blocks[0], crossed[0]]
    new = sub_blocks[1:-quarter] + crossed[1:-quarter]
    second, third = sub_blocks[-quarter:], crossed[-quarter:]
    scales, part, stats = first_sums(powers, expression, known)
    stats = [stats]
    part, new_stats = early_sums(scales, place, here, known, new, stats, part)
    stats.append(new_stats)
    part, new_stats = early_sums(scales, place, here, [], second, [], part)
    stats.append(new_stats)
    ready = known + new + second
    part = late_sums(scales, place, here, last, ready, third, stats, part)

    def hops(array, bits):
        return [array] + [from_partner(array, mask) for mask in span(bits)[1:]]

    def tree_sum(parts):
        while len(parts) > 1:
            parts = [parts[i] + parts[i + 1] for i in range(0, len(parts), 2)]
        return parts[0]

    def in_order(parts, flags):
        for up in flags:
            pairs = [(parts[i], parts[i + 1]) for i in range(0, len(parts), 2)]
            parts = [
                jnp.concatenate([jnp.where(up, high, low), jnp.where(up, low, high)])
                for low, high in pairs
            ]
        return parts[0]

    for i in range(len(far) - 1, -1, -1):
        part = tree_sum(hops(part, far[i : i + 1]))
    own, part = part, part[None]
    for i in range(0, len(near), 2):
        bits = near[i : i + 2]
        part = in_order(hops(part, bits), upper[i : i + len(bits)])
    part = in_order(hops(part, [core]), upper[-1:])

    log_degree, degree_freq, fit_slope, mean_log = fit(npower, len(lane_blocks), place, part, own)
    return log_degree, degree_freq, fit_slope[0], mean_log[0]


def solution(mesh):
    return jax.shard_map(
        on_device,
        mesh=mesh,
        in_specs=(P(AXES, None), P()),
        out_specs=(P(None, AXES), P(), P(), P()),
        check_vma=False,
    )
```
